256 devices in a mesh: loop: 256 (over z, y, x, core).
Axes of the slice: x: 4, y: 4, z: 8, core: 2. Of those that a mesh axis runs over, the one named last changes fastest.
Arguments:
- signal: float32 [256, 8192, 256], P('loop'), may hold values from -8 to 8, as said below
- tap_gain: float32 [3, 256], replicated, may hold values from 0.3 to 1.2
Outputs:
- filtered: float32 [256, 8192, 256], P('loop')
The draws below stay inside these ranges and needn't reach their ends.
Inputs may be any that keep to these rules, and one draw needn't show every extreme that they name: signal holds numbers from -8 to 8.
All inputs are finite; a program needn't handle non-finite values.
Results may differ from the reference program's by a relative error of at most 0.0003.
Values sent between devices are 32-bit elements.
A program may use at most 64 MiB of HBM per device.

```python
import jax
import jax.numpy as jnp

STEPS_DEV = 8192
CHANNELS = 256
SEGMENTS = 256


def draw_signal(key, part):
    keys = jax.random.split(key, 2)
    loud = jnp.exp(jax.random.uniform(keys[0], (SEGMENTS, 1, CHANNELS), jnp.float32, -1.2, 1.2))
    noise = jax.random.normal(keys[1], (SEGMENTS, STEPS_DEV, CHANNELS), jnp.float32)
    return jnp.clip(loud * noise, -8.0, 8.0)


def setup_inputs(seed: int = 0) -> dict:
    seeds = jax.random.split(jax.random.key(seed), 3)
    return {
        "signal": draw_signal(jax.random.fold_in(seeds[2], 71), 0),
        "tap_gain": jnp.clip(jax.random.uniform(seeds[1], (3, CHANNELS), jnp.float32, 0.3, 1.2), 0.3, 1.2),
    }


def reference(signal, tap_gain):
    wide_in = signal.astype(jnp.float32)
    mixed = tap_gain[0] * wide_in + tap_gain[1] * jnp.roll(wide_in, 33, axis=0) + tap_gain[2] * jnp.roll(wide_in, 127, axis=0)
    filtered = jnp.tanh(mixed).astype(jnp.float32)
    return filtered
```

```python
import functools

import jax
import jax.numpy as jnp
from jax import lax
from jax.experimental import pallas as pl
from jax.experimental.pallas import tpu as pltpu
from jax.sharding import PartitionSpec as P

AXIS = "loop"
NEAR, FAR = 33, 127
HOP = FAR - NEAR - NEAR
BACK_1, BACK_2 = 64, 65
PLANE = 32
NC = 16
DIVERTED = NC * 3 // 4
PARTNERS = (NEAR, HOP, BACK_1, BACK_2, 31, 2, 125)


def kernel(count, x_hbm, gain, out, x, d, g, m, q, b, relay, load_sem, send_sem,
           d_sem, g_sem, m_sem, q_sem, b_sem, relay_sem):
    me = lax.axis_index(AXIS)
    r = lax.rem(me, PLANE)
    half = x_hbm.shape[1] // 2
    cr = half // NC

    def away(steps):
        return lax.rem(me + steps + count, count)

    def cls(u):
        return lax.rem(u // 2, 2)

    ahead = cls(me)
    back = 1 - ahead
    summed = cls(away(-FAR))

    barrier = pltpu.get_barrier_semaphore()
    for steps in PARTNERS:
        for sign in (1, -1):
            pl.semaphore_signal(barrier, inc=1, device_id=away(sign * steps),
                                device_id_type=pl.DeviceIdType.LOGICAL)
    pl.semaphore_wait(barrier, 2 * len(PARTNERS))

    def rows(i):
        return pl.ds(pl.multiple_of(i * cr, cr), cr)

    def rows_of(which, i):
        return pl.ds(pl.multiple_of(which * half + i * cr, cr), cr)

    def send(src, dst, flow, sem, steps):
        pltpu.make_async_remote_copy(
            src_ref=src, dst_ref=dst, send_sem=send_sem.at[flow], recv_sem=sem,
            device_id=away(steps), device_id_type=pl.DeviceIdType.LOGICAL,
        ).start()

    def arrived(buf, sem, i):
        pltpu.make_async_copy(buf.at[rows(i)], buf.at[rows(i)], sem.at[i]).wait()

    loads = pltpu.make_async_copy(x_hbm.at[0], x, load_sem)
    n_back = jnp.where(r == 0, DIVERTED, NC)

    def first(i, carry):
        src = x_hbm.at[0, rows_of(ahead, i)]

        @pl.when(r == PLANE - 1)
        def _():
            send(src, relay.at[rows(i)], 0, relay_sem.at[i], 1 - PLANE)

        @pl.when(r != PLANE - 1)
        def _():
            send(src, d.at[rows(i)], 0, d_sem.at[i], NEAR)

        other = x_hbm.at[0, rows_of(back, i)]

        @pl.when(i < n_back)
        def _():
            send(other, q.at[rows(i)], 1, q_sem.at[i], -BACK_1)

        @pl.when(i >= n_back)
        def _():
            send(other, relay.at[rows(i)], 1, relay_sem.at[i], 2)

        return carry

    lax.fori_loop(0, NC, first, 0)
    loads.start()

    def second(i, carry):
        @pl.when(r == 0)
        def _():
            arrived(relay, relay_sem, i)
            send(relay.at[rows(i)], d.at[rows(i)], 5, d_sem.at[i], 2 * PLANE)

        @pl.when((r == 2) & (i >= DIVERTED))
        def _():
            arrived(relay, relay_sem, i)
            send(relay.at[rows(i)], b.at[rows(i)], 5, b_sem.at[i], 125)

        arrived(d, d_sem, i)
        send(d.at[rows(i)], g.at[rows(i)], 2, g_sem.at[i], HOP)
        return carry

    lax.fori_loop(0, NC, second, 0)

    def turn(i, carry):
        arrived(q, q_sem, i)
        send(q.at[rows(i)], b.at[rows(i)], 3, b_sem.at[i], -BACK_2)
        return carry

    lax.fori_loop(0, n_back, turn, 0)
    loads.wait()
    g0, g1, g2 = gain[0:1, :], gain[1:2, :], gain[2:3, :]

    def merge(i, carry):
        arrived(g, g_sem, i)
        g[rows(i), :] = g2 * g[rows(i), :] + g1 * x[rows_of(back, i), :]

        @pl.when(i > 0)
        def _():
            send(g.at[rows(i - 1)], m.at[rows(i - 1)], 4, m_sem.at[i - 1], NEAR)

        return carry

    lax.fori_loop(0, NC, merge, 0)
    send(g.at[rows(NC - 1)], m.at[rows(NC - 1)], 4, m_sem.at[NC - 1], NEAR)

    def finish(i, carry):
        arrived(b, b_sem, i)
        plain = rows_of(1 - summed, i)
        out[0, plain, :] = jnp.tanh(g0 * x[plain, :] + g1 * d[rows(i), :] + g2 * b[rows(i), :])
        arrived(m, m_sem, i)
        ready = rows_of(summed, i)
        out[0, ready, :] = jnp.tanh(g0 * x[ready, :] + m[rows(i), :])
        return carry

    lax.fori_loop(0, NC, finish, 0)

    def sent(flow, n):
        size = pl.ds(0, n * cr)
        pltpu.make_async_copy(q.at[size], q.at[size], send_sem.at[flow]).wait()

    for flow in (0, 1, 2, 4):
        sent(flow, NC)

    @pl.when(r == 0)
    def _():
        sent(3, DIVERTED)
        sent(5, NC)

    @pl.when(r != 0)
    def _():
        sent(3, NC)

    @pl.when(r == 2)
    def _():
        sent(5, NC - DIVERTED)


def body(count, signal, tap_gain):
    _, steps, channels = signal.shape
    block = pltpu.VMEM((steps // 2, channels), jnp.float32)
    return pl.pallas_call(
        functools.partial(kernel, count),
        out_shape=jax.ShapeDtypeStruct(signal.shape, jnp.float32),
        in_specs=[pl.BlockSpec(memory_space=pl.ANY), pl.BlockSpec(memory_space=pltpu.VMEM)],
        out_specs=pl.BlockSpec(memory_space=pltpu.VMEM),
        scratch_shapes=[
            pltpu.VMEM((steps, channels), jnp.float32),
            block, block, block, block, block, block,
            pltpu.SemaphoreType.DMA,
            pltpu.SemaphoreType.DMA((6,)),
        ] + [pltpu.SemaphoreType.DMA((NC,))] * 6,
        compiler_params=pltpu.CompilerParams(
            collective_id=0, has_side_effects=True, vmem_limit_bytes=60 << 20
        ),
    )(signal, tap_gain)


def solution(mesh):
    count = mesh.shape[AXIS]
    return jax.shard_map(
        functools.partial(body, count),
        mesh=mesh,
        in_specs=(P(AXIS, None, None), P()),
        out_specs=P(AXIS, None, None),
        check_vma=False,
    )
```

```python
import functools

import jax
import jax.numpy as jnp
from jax import lax
from jax.experimental import pallas as pl
from jax.experimental.pallas import tpu as pltpu
from jax.sharding import PartitionSpec as P

AXIS = "loop"
NEAR, FAR = 33, 127
HOP = FAR - NEAR - NEAR
BACK_1, BACK_2 = 64, 65
PLANE = 32
NC = 16
DIVERTED = NC * 3 // 4
PARTNERS = (NEAR, HOP, BACK_1, BACK_2, 31, 2, 125)


def kernel(count, x_hbm, gain, out, x, d, g, m, q, b, relay, load_sem, send_sem,
           d_sem, g_sem, m_sem, q_sem, b_sem, relay_sem):
    me = lax.axis_index(AXIS)
    r = lax.rem(me, PLANE)
    half = x_hbm.shape[1] // 2
    cr = half // NC

    def away(steps):
        return lax.rem(me + steps + count, count)

    def cls(u):
        return lax.rem(u // 2, 2)

    ahead = cls(me)
    back = 1 - ahead
    summed = cls(away(-FAR))

    barrier = pltpu.get_barrier_semaphore()
    for steps in PARTNERS:
        for sign in (1, -1):
            pl.semaphore_signal(barrier, inc=1, device_id=away(sign * steps),
                                device_id_type=pl.DeviceIdType.LOGICAL)
    pl.semaphore_wait(barrier, 2 * len(PARTNERS))

    def rows(i):
        return pl.ds(pl.multiple_of(i * cr, cr), cr)

    def rows_of(which, i):
        return pl.ds(pl.multiple_of(which * half + i * cr, cr), cr)

    def send(src, dst, flow, sem, steps):
        pltpu.make_async_remote_copy(
            src_ref=src, dst_ref=dst, send_sem=send_sem.at[flow], recv_sem=sem,
            device_id=away(steps), device_id_type=pl.DeviceIdType.LOGICAL,
        ).start()

    def arrived(buf, sem, i):
        pltpu.make_async_copy(buf.at[rows(i)], buf.at[rows(i)], sem.at[i]).wait()

    loads = pltpu.make_async_copy(x_hbm.at[0], x, load_sem)
    n_back = jnp.where(r == 0, DIVERTED, NC)

    def backward(i, carry):
        other = x_hbm.at[0, rows_of(back, i)]

        @pl.when(i < n_back)
        def _():
            send(other, q.at[rows(i)], 1, q_sem.at[i], -BACK_1)

        @pl.when(i >= n_back)
        def _():
            send(other, relay.at[rows(i)], 1, relay_sem.at[i], 2)

        return carry

    def forward(i, carry):
        src = x_hbm.at[0, rows_of(ahead, i)]

        @pl.when(r == PLANE - 1)
        def _():
            send(src, relay.at[rows(i)], 0, relay_sem.at[i], 1 - PLANE)

        @pl.when(r != PLANE - 1)
        def _():
            send(src, d.at[rows(i)], 0, d_sem.at[i], NEAR)

        @pl.when(r == 0)
        def _():
            arrived(relay, relay_sem, i)
            send(relay.at[rows(i)], d.at[rows(i)], 5, d_sem.at[i], 2 * PLANE)

        @pl.when((r == 2) & (i >= DIVERTED))
        def _():
            arrived(relay, relay_sem, i)
            send(relay.at[rows(i)], b.at[rows(i)], 5, b_sem.at[i], 125)

        return carry

    def onward(i, carry):
        arrived(d, d_sem, i)
        send(d.at[rows(i)], g.at[rows(i)], 2, g_sem.at[i], HOP)

        @pl.when(i < n_back)
        def _():
            arrived(q, q_sem, i)
            send(q.at[rows(i)], b.at[rows(i)], 3, b_sem.at[i], -BACK_2)

        return carry

    lax.fori_loop(0, NC, backward, 0)
    lax.fori_loop(0, NC, forward, 0)
    loads.start()
    lax.fori_loop(0, NC, onward, 0)
    loads.wait()
    g0, g1, g2 = gain[0:1, :], gain[1:2, :], gain[2:3, :]

    def merge(i, carry):
        arrived(g, g_sem, i)
        g[rows(i), :] = g2 * g[rows(i), :] + g1 * x[rows_of(back, i), :]

        @pl.when(i > 0)
        def _():
            send(g.at[rows(i - 1)], m.at[rows(i - 1)], 4, m_sem.at[i - 1], NEAR)

        return carry

    lax.fori_loop(0, NC, merge, 0)
    send(g.at[rows(NC - 1)], m.at[rows(NC - 1)], 4, m_sem.at[NC - 1], NEAR)

    def finish(i, carry):
        arrived(b, b_sem, i)
        plain = rows_of(1 - summed, i)
        out[0, plain, :] = jnp.tanh(g0 * x[plain, :] + g1 * d[rows(i), :] + g2 * b[rows(i), :])
        arrived(m, m_sem, i)
        ready = rows_of(summed, i)
        out[0, ready, :] = jnp.tanh(g0 * x[ready, :] + m[rows(i), :])
        return carry

    lax.fori_loop(0, NC, finish, 0)

    def sent(flow, n):
        size = pl.ds(0, n * cr)
        pltpu.make_async_copy(q.at[size], q.at[size], send_sem.at[flow]).wait()

    for flow in (0, 1, 2, 4):
        sent(flow, NC)

    @pl.when(r == 0)
    def _():
        sent(3, DIVERTED)
        sent(5, NC)

    @pl.when(r != 0)
    def _():
        sent(3, NC)

    @pl.when(r == 2)
    def _():
        sent(5, NC - DIVERTED)


def body(count, signal, tap_gain):
    _, steps, channels = signal.shape
    block = pltpu.VMEM((steps // 2, channels), jnp.float32)
    return pl.pallas_call(
        functools.partial(kernel, count),
        out_shape=jax.ShapeDtypeStruct(signal.shape, jnp.float32),
        in_specs=[pl.BlockSpec(memory_space=pl.ANY), pl.BlockSpec(memory_space=pltpu.VMEM)],
        out_specs=pl.BlockSpec(memory_space=pltpu.VMEM),
        scratch_shapes=[
            pltpu.VMEM((steps, channels), jnp.float32),
            block, block, block, block, block, block,
            pltpu.SemaphoreType.DMA,
            pltpu.SemaphoreType.DMA((6,)),
        ] + [pltpu.SemaphoreType.DMA((NC,))] * 6,
        compiler_params=pltpu.CompilerParams(
            collective_id=0, has_side_effects=True, vmem_limit_bytes=60 << 20
        ),
    )(signal, tap_gain)


def solution(mesh):
    count = mesh.shape[AXIS]
    return jax.shard_map(
        functools.partial(body, count),
        mesh=mesh,
        in_specs=(P(AXIS, None, None), P()),
        out_specs=P(AXIS, None, None),
        check_vma=False,
    )
```

```python
import functools

import jax
import jax.numpy as jnp
from jax import lax
from jax.experimental import pallas as pl
from jax.experimental.pallas import tpu as pltpu
from jax.sharding import PartitionSpec as P

AXIS = "loop"
NEAR, FAR = 33, 127
HOP = FAR - NEAR - NEAR
BACK_1, BACK_2 = 64, 65
PLANE = 32
NC = 16
DIVERTED = NC * 3 // 4
PARTNERS = (NEAR, HOP, BACK_1, BACK_2, 31, 2, 125)


def kernel(count, x_hbm, gain, out, x, d, g, m, q, b, relay, load_sem, send_sem,
           d_sem, g_sem, m_sem, q_sem, b_sem, relay_sem):
    me = lax.axis_index(AXIS)
    r = lax.rem(me, PLANE)
    half = x_hbm.shape[1] // 2
    cr = half // NC

    def away(steps):
        return lax.rem(me + steps + count, count)

    def cls(u):
        return lax.rem(u // 2, 2)

    ahead = cls(me)
    back = 1 - ahead
    summed = cls(away(-FAR))

    barrier = pltpu.get_barrier_semaphore()
    for steps in PARTNERS:
        for sign in (1, -1):
            pl.semaphore_signal(barrier, inc=1, device_id=away(sign * steps),
                                device_id_type=pl.DeviceIdType.LOGICAL)
    pl.semaphore_wait(barrier, 2 * len(PARTNERS))

    def rows(i):
        return pl.ds(pl.multiple_of(i * cr, cr), cr)

    def rows_of(which, i):
        return pl.ds(pl.multiple_of(which * half + i * cr, cr), cr)

    def send(src, dst, flow, sem, steps):
        pltpu.make_async_remote_copy(
            src_ref=src, dst_ref=dst, send_sem=send_sem.at[flow], recv_sem=sem,
            device_id=away(steps), device_id_type=pl.DeviceIdType.LOGICAL,
        ).start()

    def arrived(buf, sem, i):
        pltpu.make_async_copy(buf.at[rows(i)], buf.at[rows(i)], sem.at[i]).wait()

    loads = pltpu.make_async_copy(x_hbm.at[0], x, load_sem)
    n_back = jnp.where(r == 0, DIVERTED, NC)

    def backward(i, carry):
        other = x_hbm.at[0, rows_of(back, i)]

        @pl.when(i < n_back)
        def _():
            send(other, q.at[rows(i)], 1, q_sem.at[i], -BACK_1)

        @pl.when(i >= n_back)
        def _():
            send(other, relay.at[rows(i)], 1, relay_sem.at[i], 2)

        return carry

    def forward(i, carry):
        src = x_hbm.at[0, rows_of(ahead, i)]

        @pl.when(r == PLANE - 1)
        def _():
            send(src, relay.at[rows(i)], 0, relay_sem.at[i], 1 - PLANE)

        @pl.when(r != PLANE - 1)
        def _():
            send(src, d.at[rows(i)], 0, d_sem.at[i], NEAR)

        @pl.when(r == 0)
        def _():
            arrived(relay, relay_sem, i)
            send(relay.at[rows(i)], d.at[rows(i)], 5, d_sem.at[i], 2 * PLANE)

        @pl.when((r == 2) & (i >= DIVERTED))
        def _():
            arrived(relay, relay_sem, i)
            send(relay.at[rows(i)], b.at[rows(i)], 5, b_sem.at[i], 125)

        return carry

    def onward(i, carry):
        arrived(d, d_sem, i)
        send(d.at[rows(i)], g.at[rows(i)], 2, g_sem.at[i], HOP)

        @pl.when(i < n_back)
        def _():
            arrived(q, q_sem, i)
            send(q.at[rows(i)], b.at[rows(i)], 3, b_sem.at[i], -BACK_2)

        return carry

    lax.fori_loop(0, NC, backward, 0)
    lax.fori_loop(0, NC, forward, 0)
    loads.start()
    lax.fori_loop(0, NC, onward, 0)
    loads.wait()
    g0, g1, g2 = gain[0:1, :], gain[1:2, :], gain[2:3, :]

    def merge(i, carry):
        arrived(g, g_sem, i)
        g[rows(i), :] = g2 * g[rows(i), :] + g1 * x[rows_of(back, i), :]

        @pl.when(i > 0)
        def _():
            send(g.at[rows(i - 1)], m.at[rows(i - 1)], 4, m_sem.at[i - 1], NEAR)

        return carry

    lax.fori_loop(0, NC, merge, 0)
    send(g.at[rows(NC - 1)], m.at[rows(NC - 1)], 4, m_sem.at[NC - 1], NEAR)

    def finish(i, carry):
        arrived(b, b_sem, i)
        plain = rows_of(1 - summed, i)
        out[0, plain, :] = jnp.tanh(g0 * x[plain, :] + g1 * d[rows(i), :] + g2 * b[rows(i), :])
        arrived(m, m_sem, i)
        ready = rows_of(summed, i)
        out[0, ready, :] = jnp.tanh(g0 * x[ready, :] + m[rows(i), :])
        return carry

    lax.fori_loop(0, NC, finish, 0)

    def sent(flow, n):
        size = pl.ds(0, n * cr)
        pltpu.make_async_copy(q.at[size], q.at[size], send_sem.at[flow]).wait()

    for flow in (0, 1, 2, 4):
        sent(flow, NC)

    @pl.when(r == 0)
    def _():
        sent(3, DIVERTED)
        sent(5, NC)

    @pl.when(r != 0)
    def _():
        sent(3, NC)

    @pl.when(r == 2)
    def _():
        sent(5, NC - DIVERTED)


def body(count, signal, tap_gain):
    _, steps, channels = signal.shape
    block = pltpu.VMEM((steps // 2, channels), jnp.float32)
    return pl.pallas_call(
        functools.partial(kernel, count),
        out_shape=pltpu.VMEM(signal.shape, jnp.float32),
        in_specs=[pl.BlockSpec(memory_space=pl.ANY), pl.BlockSpec(memory_space=pltpu.VMEM)],
        out_specs=pl.BlockSpec(memory_space=pltpu.VMEM),
        scratch_shapes=[
            pltpu.VMEM((steps, channels), jnp.float32),
            block, block, block, block, block, block,
            pltpu.SemaphoreType.DMA,
            pltpu.SemaphoreType.DMA((6,)),
        ] + [pltpu.SemaphoreType.DMA((NC,))] * 6,
        compiler_params=pltpu.CompilerParams(
            collective_id=0, has_side_effects=True, vmem_limit_bytes=50 << 20
        ),
    )(signal, tap_gain)


def solution(mesh):
    count = mesh.shape[AXIS]
    return jax.shard_map(
        functools.partial(body, count),
        mesh=mesh,
        in_specs=(P(AXIS, None, None), P()),
        out_specs=P(AXIS, None, None),
        check_vma=False,
    )
```

```python
import functools

import jax
import jax.numpy as jnp
from jax import lax
from jax.experimental import pallas as pl
from jax.experimental.pallas import tpu as pltpu
from jax.sharding import PartitionSpec as P

AXIS = "loop"
NEAR, FAR = 33, 127
HOP = FAR - NEAR - NEAR
BACK_1, BACK_2 = 64, 65
PLANE = 32
NC = 8
DIVERTED = NC * 3 // 4
MOVED = NC // 8


def kernel(count, x_hbm, gain, out, x, d, g, m, q, b, relay, load_sem, send_sem, ready,
           d_sem, g_sem, m_sem, q_sem, b_sem, relay_sem):
    me = lax.axis_index(AXIS)
    r = lax.rem(me, PLANE)
    half = x_hbm.shape[1] // 2
    cr = half // NC

    def away(steps):
        return lax.rem(me + steps + count, count)

    def cls(u):
        return lax.rem(u // 2, 2)

    ahead = cls(me)
    back = 1 - ahead
    summed = cls(away(-FAR))

    barrier = pltpu.get_barrier_semaphore()

    def tell(sem, steps):
        pl.semaphore_signal(sem, inc=1, device_id=away(steps),
                            device_id_type=pl.DeviceIdType.LOGICAL)

    for steps in (-NEAR, BACK_1, -BACK_1, BACK_1 - HOP, BACK_2 - BACK_1):
        tell(barrier, steps)

    @pl.when(r == 0)
    def _():
        tell(barrier, PLANE - 1)
        tell(barrier, 2 - 2 * PLANE)

    @pl.when(r == 2)
    def _():
        tell(barrier, -2)
        tell(barrier, PLANE - 3)

    @pl.when(r == PLANE - 1)
    def _():
        tell(barrier, -FAR + 2)

    more = jnp.where(r == 0, 1, jnp.where((r == 2) | (r == PLANE - 1), 2, 0))
    pl.semaphore_wait(barrier, 5 + more)
    tell(ready, BACK_1)
    tell(ready, -BACK_1)

    def rows(i):
        return pl.ds(pl.multiple_of(i * cr, cr), cr)

    def rows_of(which, i):
        return pl.ds(pl.multiple_of(which * half + i * cr, cr), cr)

    def send(src, dst, flow, sem, steps):
        pltpu.make_async_remote_copy(
            src_ref=src, dst_ref=dst, send_sem=send_sem.at[flow], recv_sem=sem,
            device_id=away(steps), device_id_type=pl.DeviceIdType.LOGICAL,
        ).start()

    def arrived(buf, sem, i):
        pltpu.make_async_copy(buf.at[rows(i)], buf.at[rows(i)], sem.at[i]).wait()

    loads = pltpu.make_async_copy(x_hbm.at[0], x, load_sem)
    n_back = jnp.where(r == 0, DIVERTED, NC)

    def backward(i, carry):
        other = x_hbm.at[0, rows_of(back, i)]

        @pl.when(i < n_back)
        def _():
            send(other, q.at[rows(i)], 1, q_sem.at[i], -BACK_1)

        @pl.when(i >= n_back)
        def _():
            send(other, relay.at[rows(i)], 1, relay_sem.at[i], 2)

        return carry

    def forward(i, carry):
        src = x_hbm.at[0, rows_of(ahead, i)]

        @pl.when(r == PLANE - 1)
        def _():
            by = jnp.where(i < MOVED, 3 - PLANE, 1 - PLANE)
            send(src, relay.at[rows(i)], 0, relay_sem.at[i], by)

        @pl.when(r != PLANE - 1)
        def _():
            send(src, d.at[rows(i)], 0, d_sem.at[i], NEAR)

        @pl.when((r == 0) & (i >= MOVED))
        def _():
            arrived(relay, relay_sem, i)
            send(relay.at[rows(i)], d.at[rows(i)], 5, d_sem.at[i], 2 * PLANE)

        @pl.when((r == 2) & (i < MOVED))
        def _():
            arrived(relay, relay_sem, i)
            send(relay.at[rows(i)], d.at[rows(i)], 5, d_sem.at[i], 2 * PLANE - 2)

        @pl.when((r == 2) & (i >= DIVERTED))
        def _():
            arrived(relay, relay_sem, i)
            send(relay.at[rows(i)], b.at[rows(i)], 5, b_sem.at[i], 125)

        return carry

    def onward(i, carry):
        arrived(d, d_sem, i)
        send(d.at[rows(i)], g.at[rows(i)], 2, g_sem.at[i], HOP)

        @pl.when(i < n_back)
        def _():
            arrived(q, q_sem, i)
            send(q.at[rows(i)], b.at[rows(i)], 3, b_sem.at[i], -BACK_2)

        return carry

    lax.fori_loop(0, NC, backward, 0)
    lax.fori_loop(0, NC, forward, 0)
    loads.start()
    pl.semaphore_wait(ready, 2)
    lax.fori_loop(0, NC, onward, 0)
    loads.wait()
    g0, g1, g2 = gain[0:1, :], gain[1:2, :], gain[2:3, :]

    def merge(i, carry):
        arrived(g, g_sem, i)
        g[rows(i), :] = g2 * g[rows(i), :] + g1 * x[rows_of(back, i), :]

        @pl.when(i > 0)
        def _():
            send(g.at[rows(i - 1)], m.at[rows(i - 1)], 4, m_sem.at[i - 1], NEAR)

        return carry

    lax.fori_loop(0, NC, merge, 0)
    send(g.at[rows(NC - 1)], m.at[rows(NC - 1)], 4, m_sem.at[NC - 1], NEAR)

    def finish(i, carry):
        arrived(b, b_sem, i)
        plain = rows_of(1 - summed, i)
        out[0, plain, :] = jnp.tanh(g0 * x[plain, :] + g1 * d[rows(i), :] + g2 * b[rows(i), :])
        arrived(m, m_sem, i)
        ready = rows_of(summed, i)
        out[0, ready, :] = jnp.tanh(g0 * x[ready, :] + m[rows(i), :])
        return carry

    lax.fori_loop(0, NC, finish, 0)

    def sent(flow, n):
        size = pl.ds(0, n * cr)
        pltpu.make_async_copy(q.at[size], q.at[size], send_sem.at[flow]).wait()

    for flow in (0, 1, 2, 4):
        sent(flow, NC)

    @pl.when(r == 0)
    def _():
        sent(3, DIVERTED)
        sent(5, NC - MOVED)

    @pl.when(r != 0)
    def _():
        sent(3, NC)

    @pl.when(r == 2)
    def _():
        sent(5, NC - DIVERTED + MOVED)


def body(count, signal, tap_gain):
    _, steps, channels = signal.shape
    block = pltpu.VMEM((steps // 2, channels), jnp.float32)
    return pl.pallas_call(
        functools.partial(kernel, count),
        out_shape=pltpu.VMEM(signal.shape, jnp.float32),
        in_specs=[pl.BlockSpec(memory_space=pl.ANY), pl.BlockSpec(memory_space=pltpu.VMEM)],
        out_specs=pl.BlockSpec(memory_space=pltpu.VMEM),
        scratch_shapes=[
            pltpu.VMEM((steps, channels), jnp.float32),
            block, block, block, block, block, block,
            pltpu.SemaphoreType.DMA,
            pltpu.SemaphoreType.DMA((6,)),
            pltpu.SemaphoreType.REGULAR,
        ] + [pltpu.SemaphoreType.DMA((NC,))] * 6,
        compiler_params=pltpu.CompilerParams(
            collective_id=0, has_side_effects=True, vmem_limit_bytes=50 << 20
        ),
    )(signal, tap_gain)


def solution(mesh):
    count = mesh.shape[AXIS]
    return jax.shard_map(
        functools.partial(body, count),
        mesh=mesh,
        in_specs=(P(AXIS, None, None), P()),
        out_specs=P(AXIS, None, None),
        check_vma=False,
    )
```

```python
import functools

import jax
import jax.numpy as jnp
from jax import lax
from jax.experimental import pallas as pl
from jax.experimental.pallas import tpu as pltpu
from jax.sharding import PartitionSpec as P

AXIS = "loop"
NEAR, FAR = 33, 127
HOP = FAR - NEAR - NEAR
BACK_1, BACK_2 = 96, 33
VOUCH = 64
PLANE = 32
NC = 8
DIVERTED = NC * 3 // 4
MOVED = NC // 8


def kernel(count, x_hbm, gain, out, x, d, g, m, q, b, relay, load_sem, send_sem, ready,
           d_sem, g_sem, m_sem, q_sem, b_sem, relay_sem):
    me = lax.axis_index(AXIS)
    r = lax.rem(me, PLANE)
    half = x_hbm.shape[1] // 2
    cr = half // NC

    def away(steps):
        return lax.rem(me + steps + count, count)

    def cls(u):
        return lax.rem(u // 2, 2)

    ahead = cls(me)
    back = 1 - ahead
    summed = cls(away(-FAR))

    barrier = pltpu.get_barrier_semaphore()

    def tell(sem, steps):
        pl.semaphore_signal(sem, inc=1, device_id=away(steps),
                            device_id_type=pl.DeviceIdType.LOGICAL)

    for steps in (-NEAR, NEAR, BACK_1, VOUCH, -VOUCH, VOUCH - HOP):
        tell(barrier, steps)

    @pl.when(r == 0)
    def _():
        tell(barrier, PLANE - 1)
        tell(barrier, 2 - 2 * PLANE)

    @pl.when(r == 2)
    def _():
        tell(barrier, -2)
        tell(barrier, PLANE - 3)

    @pl.when(r == PLANE - 1)
    def _():
        tell(barrier, -FAR + 2)

    more = jnp.where(r == 0, 1, jnp.where((r == 2) | (r == PLANE - 1), 2, 0))
    pl.semaphore_wait(barrier, 6 + more)
    tell(ready, -VOUCH)

    def rows(i):
        return pl.ds(pl.multiple_of(i * cr, cr), cr)

    def rows_of(which, i):
        return pl.ds(pl.multiple_of(which * half + i * cr, cr), cr)

    def send(src, dst, flow, sem, steps):
        pltpu.make_async_remote_copy(
            src_ref=src, dst_ref=dst, send_sem=send_sem.at[flow], recv_sem=sem,
            device_id=away(steps), device_id_type=pl.DeviceIdType.LOGICAL,
        ).start()

    def arrived(buf, sem, i):
        pltpu.make_async_copy(buf.at[rows(i)], buf.at[rows(i)], sem.at[i]).wait()

    loads = pltpu.make_async_copy(x_hbm.at[0], x, load_sem)
    n_back = jnp.where(r == 0, DIVERTED, NC)

    def backward(i, carry):
        other = x_hbm.at[0, rows_of(back, i)]

        @pl.when(i < n_back)
        def _():
            send(other, q.at[rows(i)], 1, q_sem.at[i], -BACK_1)

        @pl.when(i >= n_back)
        def _():
            send(other, relay.at[rows(i)], 1, relay_sem.at[i], 2)

        return carry

    def forward(i, carry):
        src = x_hbm.at[0, rows_of(ahead, i)]

        @pl.when(r == PLANE - 1)
        def _():
            by = jnp.where(i < MOVED, 3 - PLANE, 1 - PLANE)
            send(src, relay.at[rows(i)], 0, relay_sem.at[i], by)

        @pl.when(r != PLANE - 1)
        def _():
            send(src, d.at[rows(i)], 0, d_sem.at[i], NEAR)

        @pl.when((r == 0) & (i >= MOVED))
        def _():
            arrived(relay, relay_sem, i)
            send(relay.at[rows(i)], d.at[rows(i)], 5, d_sem.at[i], 2 * PLANE)

        @pl.when((r == 2) & (i < MOVED))
        def _():
            arrived(relay, relay_sem, i)
            send(relay.at[rows(i)], d.at[rows(i)], 5, d_sem.at[i], 2 * PLANE - 2)

        @pl.when((r == 2) & (i >= DIVERTED))
        def _():
            arrived(relay, relay_sem, i)
            send(relay.at[rows(i)], b.at[rows(i)], 5, b_sem.at[i], 125)

        return carry

    def onward(i, carry):
        arrived(d, d_sem, i)
        send(d.at[rows(i)], g.at[rows(i)], 2, g_sem.at[i], HOP)

        return carry

    lax.fori_loop(0, NC, backward, 0)
    lax.fori_loop(0, NC, forward, 0)
    loads.start()
    pl.semaphore_wait(ready, 1)
    lax.fori_loop(0, NC, onward, 0)
    loads.wait()
    g0, g1, g2 = gain[0:1, :], gain[1:2, :], gain[2:3, :]

    def merge(i, carry):
        @pl.when(i < n_back)
        def _():
            arrived(q, q_sem, i)
            send(q.at[rows(i)], b.at[rows(i)], 3, b_sem.at[i], -BACK_2)

        arrived(g, g_sem, i)
        g[rows(i), :] = g2 * g[rows(i), :] + g1 * x[rows_of(back, i), :]

        @pl.when(i > 0)
        def _():
            send(g.at[rows(i - 1)], m.at[rows(i - 1)], 4, m_sem.at[i - 1], NEAR)

        return carry

    lax.fori_loop(0, NC, merge, 0)
    send(g.at[rows(NC - 1)], m.at[rows(NC - 1)], 4, m_sem.at[NC - 1], NEAR)

    def finish(i, carry):
        arrived(b, b_sem, i)
        plain = rows_of(1 - summed, i)
        out[0, plain, :] = jnp.tanh(g0 * x[plain, :] + g1 * d[rows(i), :] + g2 * b[rows(i), :])
        arrived(m, m_sem, i)
        ready = rows_of(summed, i)
        out[0, ready, :] = jnp.tanh(g0 * x[ready, :] + m[rows(i), :])
        return carry

    lax.fori_loop(0, NC, finish, 0)

    def sent(flow, n):
        size = pl.ds(0, n * cr)
        pltpu.make_async_copy(q.at[size], q.at[size], send_sem.at[flow]).wait()

    for flow in (0, 1, 2, 4):
        sent(flow, NC)

    @pl.when(r == 0)
    def _():
        sent(3, DIVERTED)
        sent(5, NC - MOVED)

    @pl.when(r != 0)
    def _():
        sent(3, NC)

    @pl.when(r == 2)
    def _():
        sent(5, NC - DIVERTED + MOVED)


def put(src, dst, sem):
    parts = 8
    size = src.shape[1] // parts
    copies = [
        pltpu.make_async_copy(
            src.at[:, pl.ds(k * size, size)], dst.at[:, pl.ds(k * size, size)], sem.at[k]
        )
        for k in range(parts)
    ]
    for copy in copies:
        copy.start()
    for copy in copies:
        copy.wait()


def body(count, signal, tap_gain):
    return pl.pallas_call(
        put,
        out_shape=jax.ShapeDtypeStruct(signal.shape, jnp.float32),
        in_specs=[pl.BlockSpec(memory_space=pltpu.VMEM)],
        out_specs=pl.BlockSpec(memory_space=pl.ANY),
        scratch_shapes=[pltpu.SemaphoreType.DMA((8,))],
        compiler_params=pltpu.CompilerParams(vmem_limit_bytes=1 << 20),
    )(filtered(count, signal, tap_gain))


def filtered(count, signal, tap_gain):
    _, steps, channels = signal.shape
    block = pltpu.VMEM((steps // 2, channels), jnp.float32)
    return pl.pallas_call(
        functools.partial(kernel, count),
        out_shape=pltpu.VMEM(signal.shape, jnp.float32),
        in_specs=[pl.BlockSpec(memory_space=pl.ANY), pl.BlockSpec(memory_space=pltpu.VMEM)],
        out_specs=pl.BlockSpec(memory_space=pltpu.VMEM),
        scratch_shapes=[
            pltpu.VMEM((steps, channels), jnp.float32),
            block, block, block, block, block, block,
            pltpu.SemaphoreType.DMA,
            pltpu.SemaphoreType.DMA((6,)),
            pltpu.SemaphoreType.REGULAR,
        ] + [pltpu.SemaphoreType.DMA((NC,))] * 6,
        compiler_params=pltpu.CompilerParams(
            collective_id=0, has_side_effects=True, vmem_limit_bytes=50 << 20
        ),
    )(signal, tap_gain)


def solution(mesh):
    count = mesh.shape[AXIS]
    return jax.shard_map(
        functools.partial(body, count),
        mesh=mesh,
        in_specs=(P(AXIS, None, None), P()),
        out_specs=P(AXIS, None, None),
        check_vma=False,
    )
```
